16 devices in a mesh: dp: 4 (over y, z, core), tp: 4 (over x).
Axes of the slice: x: 4, y: 2, z: 1, core: 2. Of those that a mesh axis runs over, the one named last changes fastest.
The devices are a block of a 4x4x8 slice.
Arguments:
- x: bfloat16 [8192, 5120], P('dp'), parts along dimension 0
- w_gate: bfloat16 [5120, 17920], P(None, 'tp')
- w_up: bfloat16 [5120, 17920], P(None, 'tp')
- w_down: bfloat16 [17920, 5120], P('tp')
Outputs:
- output: bfloat16 [8192, 5120], P('dp'), parts along dimension 0
There are 4 independent parts. The reference program is written for one: setup_inputs(seed, part) draws one part's arguments, and reference() takes and returns one part's arrays. A program takes and returns all parts, laid end to end along the dimension named above; an argument that names none is the same for every part.
All inputs are finite; a program needn't handle non-finite values.
Results may differ from the reference program's by a relative error of at most 0.016.
Values are sent between devices in bfloat16 or wider.
A program may use at most 768 MiB of HBM per device.

```python
import jax
import jax.numpy as jnp

ROWS = 2048
D = 5120
FF = 17920


def setup_inputs(seed: int = 0, part: int = 0) -> dict:
    kx, kg, ku, kd = jax.random.split(jax.random.key(seed), 4)
    drawn = {
        "x": jax.random.normal(jax.random.fold_in(kx, part), (ROWS, D), jnp.float32),
        "w_gate": jax.random.normal(kg, (D, FF), jnp.float32) * D**-0.5,
        "w_up": jax.random.normal(ku, (D, FF), jnp.float32) * D**-0.5,
        "w_down": jax.random.normal(kd, (FF, D), jnp.float32) * FF**-0.5,
    }
    return {k: v.astype(jnp.bfloat16) for k, v in drawn.items()}


def reference(x, w_gate, w_up, w_down):
    gate = jnp.dot(x, w_gate, preferred_element_type=jnp.float32)
    up = jnp.dot(x, w_up, preferred_element_type=jnp.float32)
    hidden = (jax.nn.silu(gate) * up).astype(jnp.bfloat16)
    return jnp.dot(hidden, w_down, preferred_element_type=jnp.float32).astype(jnp.bfloat16)
```

```python
import functools

import jax
import jax.numpy as jnp
from jax import lax
from jax.experimental import pallas as pl
from jax.experimental.pallas import tpu as pltpu
from jax.sharding import PartitionSpec as P

MESH = pl.DeviceIdType.MESH
F32, BF16 = jnp.float32, jnp.bfloat16

SMALL, BIG = 2, 3
UP, DOWN = 7, 4
STEPS = UP + DOWN
HOPS = 6
EVENTS = HOPS * DOWN


def block_kernel(
    n, x_hbm, wg_hbm, wu_hbm, wd_hbm, y_hbm,
    w_buf, x_buf, hid, term, stage, got,
    w_sem, x_sem, o_sem, send_sem, recv_sem,
):
    rows, dim = x_hbm.shape
    units = wg_hbm.shape[1]
    wide = dim // DOWN
    half = wide // 2
    tile = units // UP
    few = rows // 8
    many = 2 * few

    me = lax.axis_index("tp")
    group = lax.axis_index("dp")
    peers = (lax.rem(me + 1, n), lax.rem(me + n - 1, n))

    barrier = pltpu.get_barrier_semaphore()
    for peer in peers:
        pl.semaphore_signal(barrier, inc=1, device_id=(group, peer), device_id_type=MESH)

    def up_copies(s, slot):
        cols = pl.ds(pl.multiple_of(s * tile, 128), tile)
        return (
            pltpu.make_async_copy(wg_hbm.at[:, cols], w_buf.at[slot, :, pl.ds(0, tile)], w_sem.at[slot, 0]),
            pltpu.make_async_copy(wu_hbm.at[:, cols], w_buf.at[slot, :, pl.ds(tile, tile)], w_sem.at[slot, 1]),
        )

    def down_copy(s, slot):
        cols = pl.ds(pl.multiple_of(s * wide, 128), wide)
        return pltpu.make_async_copy(wd_hbm.at[:, cols], w_buf.at[slot, pl.ds(0, units), pl.ds(0, wide)], w_sem.at[slot, 0])

    def start_up(s, slot):
        for copy in up_copies(s, slot):
            copy.start()

    def x_copy(row, count):
        return pltpu.make_async_copy(x_hbm.at[pl.ds(pl.multiple_of(row, 16), count)], x_buf.at[pl.ds(0, count)], x_sem)

    def block_at(d, k):
        return lax.rem(me + 2 * n - 1 - k, n) if d == 0 else lax.rem(me + 1 + k, n)

    def y_at(d, u, k, row, high):
        start = pl.multiple_of(row + block_at(d, k) * high, 16)
        return y_hbm.at[pl.ds(start, high), pl.ds(pl.multiple_of(u * wide + d * half, 128), half)]

    def hop(d, u, k, src, dst):
        return pltpu.make_async_remote_copy(
            src_ref=src, dst_ref=dst,
            send_sem=send_sem.at[d, u, k], recv_sem=recv_sem.at[d, u, k],
            device_id=(group, peers[d]), device_id_type=MESH,
        )

    def partial_hop(d, u, k, high):
        return hop(d, u, k, stage.at[d, u, lax.rem(k, 2), pl.ds(0, high)], got.at[d, u, k, pl.ds(0, high)])

    def own_copy(d, u, row, high):
        return pltpu.make_async_copy(stage.at[d, u, 1, pl.ds(0, high)], y_at(d, u, n - 1, row, high), o_sem.at[d, u])

    def mine(d, u, k, high):
        return term[u, d, pl.ds(pl.multiple_of(block_at(d, k) * high, 16), high), :]

    def first_hop(u, high):
        for d in (0, 1):
            stage[d, u, 0, pl.ds(0, high), :] = mine(d, u, 0, high).astype(BF16)
            partial_hop(d, u, 0, high).start()

    def event(e, row, high):
        k, u = e // DOWN + 1, lax.rem(e, DOWN)

        @pl.when(k < n)
        def _():
            for d in (0, 1):
                partial_hop(d, u, k - 1, high).wait()
                total = got[d, u, k - 1, pl.ds(0, high), :].astype(F32) + mine(d, u, k, high)
                stage[d, u, lax.rem(k, 2), pl.ds(0, high), :] = total.astype(BF16)

                @pl.when(k < n - 1)
                def _():
                    partial_hop(d, u, k, high).start()

                @pl.when(k == n - 1)
                def _():
                    place = y_at(d, u, n - 1, row, high)
                    hop(d, u, n - 1, stage.at[d, u, 1, pl.ds(0, high)], place).start()
                    own_copy(d, u, row, high).start()

        @pl.when(k >= n)
        def _():
            for d in (0, 1):
                place = y_at(d, u, k, row, high)
                hop(d, u, k - 1, place, place).wait()

                @pl.when(k == n)
                def _():
                    own_copy(d, u, row, high).wait()

                @pl.when(k < HOPS)
                def _():
                    hop(d, u, k, place, place).start()

    def events(low, high_end, row, high):
        lax.fori_loop(low, high_end, lambda e, _: (event(e, row, high), 0)[1], 0)

    def one_pass(p, count, before, more):
        high = count // n

        @pl.loop(0, UP)
        def _(s):
            slot = lax.rem(p + s, 2)

            @pl.when(s < UP - 1)
            def _():
                start_up(s + 1, 1 - slot)

            @pl.when(s == UP - 1)
            def _():
                down_copy(0, 1 - slot).start()

            for copy in up_copies(s, slot):
                copy.wait()
            both = jnp.dot(x_buf[pl.ds(0, count), :], w_buf[slot], preferred_element_type=F32)
            cols = pl.ds(pl.multiple_of(s * tile, 128), tile)
            hid[pl.ds(0, count), cols] = (jax.nn.silu(both[:, :tile]) * both[:, tile:]).astype(BF16)
            before(s)

        @pl.loop(0, DOWN)
        def _(u):
            slot = lax.rem(p + UP + u, 2)

            @pl.when(u < DOWN - 1)
            def _():
                down_copy(u + 1, 1 - slot).start()

            @pl.when(u == DOWN - 1)
            def _():
                more(1 - slot)

            down_copy(u, slot).wait()
            out = jnp.dot(hid[pl.ds(0, count), :], w_buf[slot, pl.ds(0, units), :], preferred_element_type=F32)
            term[u, 0, pl.ds(0, count), :] = out[:, :half]
            term[u, 1, pl.ds(0, count), :] = out[:, half:]
            first_hop(u, high)
            before(u + UP)

    x_copy(0, few).start()
    start_up(0, 0)
    pl.semaphore_wait(barrier, 2)

    @pl.loop(0, SMALL)
    def _(p):
        x_copy(p * few, few).wait()

        def before(t):
            @pl.when(p > 0)
            def _():
                events(EVENTS * t // STEPS, EVENTS * (t + 1) // STEPS, (p - 1) * few, few // n)

        def more(slot):
            start_up(0, slot)

            @pl.when(p < SMALL - 1)
            def _():
                x_copy((p + 1) * few, few).start()

            @pl.when(p == SMALL - 1)
            def _():
                x_copy(SMALL * few, many).start()

        one_pass(p, few, before, more)

    @pl.loop(0, BIG)
    def _(q):
        row = SMALL * few + q * many
        x_copy(row, many).wait()

        def before(t):
            @pl.when((q == 0) & (t < HOPS))
            def _():
                events(DOWN * t, DOWN * (t + 1), (SMALL - 1) * few, few // n)

            @pl.when(q > 0)
            def _():
                events(EVENTS * t // STEPS, EVENTS * (t + 1) // STEPS, row - many, many // n)

        def more(slot):
            @pl.when(q < BIG - 1)
            def _():
                start_up(0, slot)
                x_copy(row + many, many).start()

        one_pass(SMALL + q, many, before, more)

    events(0, EVENTS, SMALL * few + (BIG - 1) * many, many // n)


PIECES = 8


def copy_kernel(y_hbm, out_hbm, buf, in_sem, out_sem):
    high = y_hbm.shape[0] // PIECES
    into = [pltpu.make_async_copy(y_hbm.at[pl.ds(i * high, high)], buf.at[i], in_sem.at[i]) for i in range(PIECES)]
    back = [pltpu.make_async_copy(buf.at[i], out_hbm.at[pl.ds(i * high, high)], out_sem.at[i]) for i in range(PIECES)]
    for copy in into:
        copy.start()
    for i in range(PIECES):
        into[i].wait()
        back[i].start()
    for copy in back:
        copy.wait()


def solution(mesh):
    n = mesh.shape["tp"]

    def step(x, w_gate, w_up, w_down):
        rows, dim = x.shape
        units = w_gate.shape[1]
        many, wide, tile = rows // 4, dim // DOWN, units // UP
        half, high = wide // 2, rows // 4 // n
        anywhere = pl.BlockSpec(memory_space=pl.ANY)
        y = pl.pallas_call(
            functools.partial(block_kernel, n),
            out_shape=jax.ShapeDtypeStruct((rows, dim), BF16),
            in_specs=[anywhere] * 4,
            out_specs=anywhere,
            scratch_shapes=[
                pltpu.VMEM((2, dim, max(wide, 2 * tile)), BF16),
                pltpu.VMEM((many, dim), BF16),
                pltpu.VMEM((many, units), BF16),
                pltpu.VMEM((DOWN, 2, many, half), F32),
                pltpu.VMEM((2, DOWN, 2, high, half), BF16),
                pltpu.VMEM((2, DOWN, n - 1, high, half), BF16),
                pltpu.SemaphoreType.DMA((2, 2)),
                pltpu.SemaphoreType.DMA,
                pltpu.SemaphoreType.DMA((2, DOWN)),
                pltpu.SemaphoreType.DMA((2, DOWN, HOPS)),
                pltpu.SemaphoreType.DMA((2, DOWN, HOPS)),
            ],
            compiler_params=pltpu.CompilerParams(
                collective_id=0, has_side_effects=True, vmem_limit_bytes=67043328
            ),
            name="block",
        )(x, w_gate, w_up, w_down)
        return pl.pallas_call(
            copy_kernel,
            out_shape=jax.ShapeDtypeStruct((rows, dim), BF16),
            in_specs=[anywhere],
            out_specs=anywhere,
            scratch_shapes=[
                pltpu.VMEM((PIECES, rows // PIECES, dim), BF16),
                pltpu.SemaphoreType.DMA((PIECES,)),
                pltpu.SemaphoreType.DMA((PIECES,)),
            ],
            compiler_params=pltpu.CompilerParams(vmem_limit_bytes=40 << 20),
            name="place",
        )(y)

    return jax.shard_map(
        step,
        mesh=mesh,
        in_specs=(P("dp", None), P(None, "tp"), P(None, "tp"), P("tp", None)),
        out_specs=P("dp", None),
        check_vma=False,
    )
```

```python
import functools

import jax
import jax.numpy as jnp
from jax import lax
from jax.experimental import pallas as pl
from jax.experimental.pallas import tpu as pltpu
from jax.sharding import PartitionSpec as P

MESH = pl.DeviceIdType.MESH
F32, BF16 = jnp.float32, jnp.bfloat16

SECTIONS = ((1, 4), (5, 5), (1, 3))
PASSES = sum(times for times, _ in SECTIONS)
LARGEST = max(size for _, size in SECTIONS)
SLOTS = 3
UP, DOWN = 7, 4
STEPS = UP + DOWN
HOPS = 6
PLAN = {
    1: ((1, 0),), 2: ((1, 1),), 3: ((2, 0),), 4: ((1, 2), (1, 3), (2, 1)), 5: ((2, 2), (3, 0)), 6: ((2, 3), (3, 1)),
    7: ((4, 0), (3, 2)), 8: ((3, 3), (4, 1)), 9: ((5, 0), (4, 2)), 10: ((4, 3), (5, 1)), 11: ((5, 2),),
    12: ((6, 0), (5, 3)), 13: ((6, 2),), 14: ((6, 1), (6, 3)),
}


def block_kernel(
    n, x_hbm, wg_hbm, wu_hbm, wd_hbm, y_hbm,
    w_buf, x_buf, hid, term, stage, got,
    w_sem, x_sem, o_sem, send_sem, recv_sem,
):
    rows, dim = x_hbm.shape
    units = wg_hbm.shape[1]
    wide = dim // DOWN
    half = wide // 2
    tile = units // UP
    part = rows // sum(times * size for times, size in SECTIONS)

    me = lax.axis_index("tp")
    group = lax.axis_index("dp")
    peers = (lax.rem(me + 1, n), lax.rem(me + n - 1, n))

    barrier = pltpu.get_barrier_semaphore()
    for peer in peers:
        pl.semaphore_signal(barrier, inc=1, device_id=(group, peer), device_id_type=MESH)

    def up_copies(s, slot):
        cols = pl.ds(pl.multiple_of(s * tile, 128), tile)
        return (
            pltpu.make_async_copy(wg_hbm.at[:, cols], w_buf.at[slot, :, pl.ds(0, tile)], w_sem.at[slot, 0]),
            pltpu.make_async_copy(wu_hbm.at[:, cols], w_buf.at[slot, :, pl.ds(tile, tile)], w_sem.at[slot, 1]),
        )

    def down_copy(s, slot):
        cols = pl.ds(pl.multiple_of(s * wide, 128), wide)
        return pltpu.make_async_copy(wd_hbm.at[:, cols], w_buf.at[slot, pl.ds(0, units), pl.ds(0, wide)], w_sem.at[slot, 0])

    def start_up(s, slot):
        for copy in up_copies(s, slot):
            copy.start()

    def x_copy(row, count):
        return pltpu.make_async_copy(x_hbm.at[pl.ds(pl.multiple_of(row, 16), count)], x_buf.at[pl.ds(0, count)], x_sem)

    def block_at(d, k):
        return lax.rem(me + 2 * n - 1 - k, n) if d == 0 else lax.rem(me + 1 + k, n)

    def y_at(d, u, k, row, high):
        start = pl.multiple_of(row + block_at(d, k) * high, 16)
        return y_hbm.at[pl.ds(start, high), pl.ds(pl.multiple_of(u * wide + d * half, 128), half)]

    def hop(d, u, k, src, dst):
        return pltpu.make_async_remote_copy(
            src_ref=src, dst_ref=dst,
            send_sem=send_sem.at[d, u, k], recv_sem=recv_sem.at[d, u, k],
            device_id=(group, peers[d]), device_id_type=MESH,
        )

    def partial_hop(d, u, k, high):
        return hop(d, u, k, stage.at[d, u, k % 2, pl.ds(0, high)], got.at[d, u, k, pl.ds(0, high)])

    def own_copy(d, u, row, high):
        return pltpu.make_async_copy(stage.at[d, u, 1, pl.ds(0, high)], y_at(d, u, n - 1, row, high), o_sem.at[d, u])

    def mine(d, u, k, high):
        return term[u, d, pl.ds(pl.multiple_of(block_at(d, k) * high, 16), high), :]

    def first_hop(u, high):
        for d in (0, 1):
            stage[d, u, 0, pl.ds(0, high), :] = mine(d, u, 0, high).astype(BF16)
            partial_hop(d, u, 0, high).start()

    def event(k, u, row, high):
        for d in (0, 1):
            if k < n:
                partial_hop(d, u, k - 1, high).wait()
                total = got[d, u, k - 1, pl.ds(0, high), :].astype(F32) + mine(d, u, k, high)
                stage[d, u, k % 2, pl.ds(0, high), :] = total.astype(BF16)
                if k < n - 1:
                    partial_hop(d, u, k, high).start()
                else:
                    hop(d, u, k, stage.at[d, u, k % 2, pl.ds(0, high)], y_at(d, u, k, row, high)).start()
                    own_copy(d, u, row, high).start()
            else:
                place = y_at(d, u, k, row, high)
                hop(d, u, k - 1, place, place).wait()
                if k == n:
                    own_copy(d, u, row, high).wait()
                if k < HOPS:
                    hop(d, u, k, place, place).start()

    def events(after, row, high):
        for k, u in PLAN.get(after, ()):
            event(k, u, row, high)

    x_copy(0, SECTIONS[0][1] * part).start()
    start_up(0, 0)
    start_up(1, 1)
    pl.semaphore_wait(barrier, 2)

    def section(i, first_pass, first_row):
        times, size = SECTIONS[i]
        count = size * part
        high = count // n
        final = i == len(SECTIONS) - 1

        @pl.loop(0, times)
        def _(p):
            row = first_row + p * count
            step = STEPS * (first_pass + p)

            def last_pass_events(t):
                @pl.when(p > 0)
                def _():
                    events(t + DOWN, row - count, high)

                if i > 0:
                    before = SECTIONS[i - 1][1] * part

                    @pl.when(p == 0)
                    def _():
                        events(t + DOWN, row - before, before // n)

            x_copy(row, count).wait()

            @pl.loop(0, UP)
            def _(s):
                slot = lax.rem(step + s, SLOTS)
                ahead = lax.rem(slot + 2, SLOTS)

                @pl.when(s < UP - 2)
                def _():
                    start_up(s + 2, ahead)

                @pl.when(s >= UP - 2)
                def _():
                    down_copy(s + 2 - UP, ahead).start()

                for copy in up_copies(s, slot):
                    copy.wait()
                both = jnp.dot(x_buf[pl.ds(0, count), :], w_buf[slot], preferred_element_type=F32)
                cols = pl.ds(pl.multiple_of(s * tile, 128), tile)
                hid[pl.ds(0, count), cols] = (jax.nn.silu(both[:, :tile]) * both[:, tile:]).astype(BF16)
                for t in range(UP):

                    @pl.when(s == t)
                    def _():
                        last_pass_events(t)

            @pl.loop(0, DOWN)
            def _(u):
                slot = lax.rem(step + UP + u, SLOTS)
                ahead = lax.rem(slot + 2, SLOTS)
                more = p < times - 1 if final else True

                @pl.when(u < DOWN - 2)
                def _():
                    down_copy(u + 2, ahead).start()

                @pl.when((u >= DOWN - 2) & more)
                def _():
                    start_up(u + 2 - DOWN, ahead)

                @pl.when((u == 0) & (p < times - 1))
                def _():
                    x_copy(row + count, count).start()

                if not final:

                    @pl.when((u == 0) & (p == times - 1))
                    def _():
                        x_copy(row + count, SECTIONS[i + 1][1] * part).start()

                down_copy(u, slot).wait()
                out = jnp.dot(hid[pl.ds(0, count), :], w_buf[slot, pl.ds(0, units), :], preferred_element_type=F32)
                term[u, 0, pl.ds(0, count), :] = out[:, :half]
                term[u, 1, pl.ds(0, count), :] = out[:, half:]
                first_hop(u, high)
                for t in range(DOWN):

                    @pl.when(u == t)
                    def _():
                        last_pass_events(UP + t)
                        events(t, row, high)

        return first_pass + times, first_row + times * count

    place = (0, 0)
    for i in range(len(SECTIONS)):
        place = section(i, *place)
    count = SECTIONS[-1][1] * part
    for after in range(DOWN, max(PLAN) + 1):
        events(after, rows - count, count // n)


PIECES = 8


def copy_kernel(y_hbm, out_hbm, buf, in_sem, out_sem):
    high = y_hbm.shape[0] // PIECES
    into = [pltpu.make_async_copy(y_hbm.at[pl.ds(i * high, high)], buf.at[i], in_sem.at[i]) for i in range(PIECES)]
    back = [pltpu.make_async_copy(buf.at[i], out_hbm.at[pl.ds(i * high, high)], out_sem.at[i]) for i in range(PIECES)]
    for copy in into:
        copy.start()
    for copy in into:
        copy.wait()
    for copy in back:
        copy.start()
    for copy in back:
        copy.wait()


def solution(mesh):
    n = mesh.shape["tp"]

    def step(x, w_gate, w_up, w_down):
        rows, dim = x.shape
        units = w_gate.shape[1]
        part = rows // sum(times * size for times, size in SECTIONS)
        count, wide, tile = LARGEST * part, dim // DOWN, units // UP
        half, high = wide // 2, count // n
        anywhere = pl.BlockSpec(memory_space=pl.ANY)
        y = pl.pallas_call(
            functools.partial(block_kernel, n),
            out_shape=jax.ShapeDtypeStruct((rows, dim), BF16),
            in_specs=[anywhere] * 4,
            out_specs=anywhere,
            scratch_shapes=[
                pltpu.VMEM((SLOTS, dim, max(wide, 2 * tile)), BF16),
                pltpu.VMEM((count, dim), BF16),
                pltpu.VMEM((count, units), BF16),
                pltpu.VMEM((DOWN, 2, count, half), F32),
                pltpu.VMEM((2, DOWN, 2, high, half), BF16),
                pltpu.VMEM((2, DOWN, n - 1, high, half), BF16),
                pltpu.SemaphoreType.DMA((SLOTS, 2)),
                pltpu.SemaphoreType.DMA,
                pltpu.SemaphoreType.DMA((2, DOWN)),
                pltpu.SemaphoreType.DMA((2, DOWN, HOPS)),
                pltpu.SemaphoreType.DMA((2, DOWN, HOPS)),
            ],
            compiler_params=pltpu.CompilerParams(
                collective_id=0, has_side_effects=True, vmem_limit_bytes=67043328
            ),
            name="block",
        )(x, w_gate, w_up, w_down)
        return pl.pallas_call(
            copy_kernel,
            out_shape=jax.ShapeDtypeStruct((rows, dim), BF16),
            in_specs=[anywhere],
            out_specs=anywhere,
            scratch_shapes=[
                pltpu.VMEM((PIECES, rows // PIECES, dim), BF16),
                pltpu.SemaphoreType.DMA((PIECES,)),
                pltpu.SemaphoreType.DMA((PIECES,)),
            ],
            compiler_params=pltpu.CompilerParams(vmem_limit_bytes=40 << 20),
            name="place",
        )(y)

    return jax.shard_map(
        step,
        mesh=mesh,
        in_specs=(P("dp", None), P(None, "tp"), P(None, "tp"), P("tp", None)),
        out_specs=P("dp", None),
        check_vma=False,
    )
```

```python
import functools

import jax
import jax.numpy as jnp
from jax import lax
from jax.experimental import pallas as pl
from jax.experimental.pallas import tpu as pltpu
from jax.sharding import PartitionSpec as P

MESH = pl.DeviceIdType.MESH
F32, BF16 = jnp.float32, jnp.bfloat16

SECTIONS = ((1, 4), (5, 5), (1, 3))
PASSES = sum(times for times, _ in SECTIONS)
LARGEST = max(size for _, size in SECTIONS)
SLOTS = 2
LEAD = SLOTS - 1
BLOCK_VMEM, PLACE_VMEM = 38 << 20, 8 << 20
UP, DOWN = 7, 4
STEPS = UP + DOWN
HOPS = 6
PLAN = {
    1: ((1, 0),), 2: ((1, 1),), 3: ((2, 0),), 4: ((1, 2), (1, 3), (2, 1)), 5: ((2, 2), (3, 0)), 6: ((2, 3), (3, 1)),
    7: ((4, 0), (3, 2)), 8: ((3, 3), (4, 1)), 9: ((5, 0), (4, 2)), 10: ((4, 3), (5, 1)), 11: ((5, 2),),
    12: ((6, 0), (5, 3)), 13: ((6, 2),), 14: ((6, 1), (6, 3)),
}


def block_kernel(
    n, x_hbm, wg_hbm, wu_hbm, wd_hbm, y_hbm, w_buf,
    x_buf, hid, term, stage, got,
    w_sem, x_sem, o_sem, send_sem, recv_sem, hold_sem,
):
    rows, dim = x_hbm.shape
    units = wg_hbm.shape[1]
    wide = dim // DOWN
    half = wide // 2
    tile = units // UP
    part = rows // sum(times * size for times, size in SECTIONS)

    me = lax.axis_index("tp")
    group = lax.axis_index("dp")
    peers = (lax.rem(me + 1, n), lax.rem(me + n - 1, n))

    barrier = pltpu.get_barrier_semaphore()
    for peer in peers:
        pl.semaphore_signal(barrier, inc=1, device_id=(group, peer), device_id_type=MESH)

    def up_copies(s, slot):
        cols = pl.ds(pl.multiple_of(s * tile, 128), tile)
        return (
            pltpu.make_async_copy(wg_hbm.at[:, cols], w_buf.at[slot, :, pl.ds(0, tile)], w_sem.at[slot, 0]),
            pltpu.make_async_copy(wu_hbm.at[:, cols], w_buf.at[slot, :, pl.ds(tile, tile)], w_sem.at[slot, 1]),
        )

    def down_copy(s, slot):
        cols = pl.ds(pl.multiple_of(s * wide, 128), wide)
        return pltpu.make_async_copy(wd_hbm.at[:, cols], w_buf.at[slot, pl.ds(0, units), pl.ds(0, wide)], w_sem.at[slot, 0])

    def start_up(s, slot):
        for copy in up_copies(s, slot):
            copy.start()

    def x_copy(row, count):
        return pltpu.make_async_copy(x_hbm.at[pl.ds(pl.multiple_of(row, 16), count)], x_buf.at[pl.ds(0, count)], x_sem)

    def block_at(d, k):
        return lax.rem(me + 2 * n - 1 - k, n) if d == 0 else lax.rem(me + 1 + k, n)

    def y_at(d, u, k, row, high):
        start = pl.multiple_of(row + block_at(d, k) * high, 16)
        return y_hbm.at[pl.ds(start, high), pl.ds(pl.multiple_of(u * wide + d * half, 128), half)]

    def hop(d, u, k, src, dst):
        return pltpu.make_async_remote_copy(
            src_ref=src, dst_ref=dst,
            send_sem=send_sem.at[d, u, k], recv_sem=recv_sem.at[d, u, k],
            device_id=(group, peers[d]), device_id_type=MESH,
        )

    def partial_hop(d, u, k, high):
        return hop(d, u, k, stage.at[d, u, k % 2, pl.ds(0, high)], got.at[d, u, k, pl.ds(0, high)])

    def own_copy(d, u, row, high):
        return pltpu.make_async_copy(stage.at[d, u, 1, pl.ds(0, high)], y_at(d, u, n - 1, row, high), o_sem.at[d, u])

    def mine(d, u, k, high):
        return term[u, d, pl.ds(pl.multiple_of(block_at(d, k) * high, 16), high), :]

    def first_hop(u, high):
        for d in (0, 1):
            stage[d, u, 0, pl.ds(0, high), :] = mine(d, u, 0, high).astype(BF16)
            partial_hop(d, u, 0, high).start()

    def event(k, u, row, high):
        for d in (0, 1):
            if k < n:
                partial_hop(d, u, k - 1, high).wait()
                total = got[d, u, k - 1, pl.ds(0, high), :].astype(F32) + mine(d, u, k, high)
                stage[d, u, k % 2, pl.ds(0, high), :] = total.astype(BF16)
                if k < n - 1:
                    partial_hop(d, u, k, high).start()
                else:
                    hop(d, u, k, stage.at[d, u, k % 2, pl.ds(0, high)], y_at(d, u, k, row, high)).start()
                    own_copy(d, u, row, high).start()
            else:
                place = y_at(d, u, k, row, high)
                hop(d, u, k - 1, place, place).wait()
                if k == n:
                    own_copy(d, u, row, high).wait()
                if k < HOPS:
                    hop(d, u, k, place, place).start()

    def events(after, row, high):
        for k, u in PLAN.get(after, ()):
            event(k, u, row, high)

    x_copy(0, SECTIONS[0][1] * part).start()
    for i in range(LEAD):
        start_up(i, i)
    pl.semaphore_wait(barrier, 2)

    def section(i, first_pass, first_row):
        times, size = SECTIONS[i]
        count = size * part
        high = count // n
        final = i == len(SECTIONS) - 1

        @pl.loop(0, times)
        def _(p):
            row = first_row + p * count
            step = STEPS * (first_pass + p)

            def last_pass_events(t):
                @pl.when(p > 0)
                def _():
                    events(t + DOWN, row - count, high)

                if i > 0:
                    before = SECTIONS[i - 1][1] * part

                    @pl.when(p == 0)
                    def _():
                        events(t + DOWN, row - before, before // n)

            x_copy(row, count).wait()

            @pl.loop(0, UP)
            def _(s):
                slot = lax.rem(step + s, SLOTS)
                ahead = lax.rem(slot + LEAD, SLOTS)

                @pl.when(s < UP - LEAD)
                def _():
                    start_up(s + LEAD, ahead)

                @pl.when(s >= UP - LEAD)
                def _():
                    down_copy(s + LEAD - UP, ahead).start()

                for copy in up_copies(s, slot):
                    copy.wait()
                both = jnp.dot(x_buf[pl.ds(0, count), :], w_buf[slot], preferred_element_type=F32)
                cols = pl.ds(pl.multiple_of(s * tile, 128), tile)
                hid[pl.ds(0, count), cols] = (jax.nn.silu(both[:, :tile]) * both[:, tile:]).astype(BF16)
                for t in range(UP):

                    @pl.when(s == t)
                    def _():
                        last_pass_events(t)

            @pl.loop(0, DOWN)
            def _(u):
                slot = lax.rem(step + UP + u, SLOTS)
                ahead = lax.rem(slot + LEAD, SLOTS)
                more = p < times - 1 if final else True

                @pl.when(u < DOWN - LEAD)
                def _():
                    down_copy(u + LEAD, ahead).start()

                @pl.when((u >= DOWN - LEAD) & more)
                def _():
                    start_up(u + LEAD - DOWN, ahead)

                @pl.when((u == 0) & (p < times - 1))
                def _():
                    x_copy(row + count, count).start()

                if not final:

                    @pl.when((u == 0) & (p == times - 1))
                    def _():
                        x_copy(row + count, SECTIONS[i + 1][1] * part).start()

                down_copy(u, slot).wait()
                out = jnp.dot(hid[pl.ds(0, count), :], w_buf[slot, pl.ds(0, units), :], preferred_element_type=F32)
                term[u, 0, pl.ds(0, count), :] = out[:, :half]
                term[u, 1, pl.ds(0, count), :] = out[:, half:]
                first_hop(u, high)
                for t in range(DOWN):

                    @pl.when(u == t)
                    def _():
                        last_pass_events(UP + t)
                        events(t, row, high)

        return first_pass + times, first_row + times * count

    place = (0, 0)
    for i in range(len(SECTIONS)):
        place = section(i, *place)
    count = SECTIONS[-1][1] * part
    ready = rows - count
    copies = [
        pltpu.make_async_copy(
            y_hbm.at[pl.ds(0, ready), pl.ds(c * wide, wide)], held(w_buf, c, rows, ready, wide), hold_sem.at[c]
        )
        for c in range(DOWN)
    ]
    for copy in copies:
        copy.start()
    for after in range(DOWN, max(PLAN) + 1):
        events(after, rows - count, count // n)
    for copy in copies:
        copy.wait()


def held(w_buf, c, rows, ready, wide):
    return w_buf.at[c // 2, pl.ds(c % 2 * rows, ready), pl.ds(0, wide)]


def place_kernel(y_hbm, w_buf, out_hbm, last, in_sem, out_sem):
    rows, dim = y_hbm.shape
    wide = dim // DOWN
    ready = rows - last.shape[0]
    into = pltpu.make_async_copy(y_hbm.at[pl.ds(ready, rows - ready)], last, in_sem)
    into.start()
    back = [
        pltpu.make_async_copy(
            held(w_buf, c, rows, ready, wide), out_hbm.at[pl.ds(0, ready), pl.ds(c * wide, wide)], out_sem.at[c]
        )
        for c in range(DOWN)
    ]
    back.append(pltpu.make_async_copy(last, out_hbm.at[pl.ds(ready, rows - ready)], out_sem.at[DOWN]))
    for copy in back[:-1]:
        copy.start()
    into.wait()
    back[-1].start()
    for copy in back:
        copy.wait()


def solution(mesh):
    n = mesh.shape["tp"]

    def step(x, w_gate, w_up, w_down):
        rows, dim = x.shape
        units = w_gate.shape[1]
        part = rows // sum(times * size for times, size in SECTIONS)
        count, wide, tile = LARGEST * part, dim // DOWN, units // UP
        half, high = wide // 2, count // n
        anywhere = pl.BlockSpec(memory_space=pl.ANY)
        weights = (SLOTS, dim, max(wide, 2 * tile))
        in_vmem = pl.BlockSpec(memory_space=pltpu.VMEM)
        y, kept = pl.pallas_call(
            functools.partial(block_kernel, n),
            out_shape=(jax.ShapeDtypeStruct((rows, dim), BF16), pltpu.VMEM(weights, BF16)),
            in_specs=[anywhere] * 4,
            out_specs=(anywhere, in_vmem),
            scratch_shapes=[
                pltpu.VMEM((count, dim), BF16),
                pltpu.VMEM((count, units), BF16),
                pltpu.VMEM((DOWN, 2, count, half), F32),
                pltpu.VMEM((2, DOWN, 2, high, half), BF16),
                pltpu.VMEM((2, DOWN, n - 1, high, half), BF16),
                pltpu.SemaphoreType.DMA((SLOTS, 2)),
                pltpu.SemaphoreType.DMA,
                pltpu.SemaphoreType.DMA((2, DOWN)),
                pltpu.SemaphoreType.DMA((2, DOWN, HOPS)),
                pltpu.SemaphoreType.DMA((2, DOWN, HOPS)),
                pltpu.SemaphoreType.DMA((DOWN,)),
            ],
            compiler_params=pltpu.CompilerParams(
                collective_id=0, has_side_effects=True, vmem_limit_bytes=BLOCK_VMEM
            ),
            name="block",
        )(x, w_gate, w_up, w_down)
        return pl.pallas_call(
            place_kernel,
            out_shape=jax.ShapeDtypeStruct((rows, dim), BF16),
            in_specs=[anywhere, anywhere],
            out_specs=anywhere,
            scratch_shapes=[
                pltpu.VMEM((SECTIONS[-1][1] * part, dim), BF16),
                pltpu.SemaphoreType.DMA,
                pltpu.SemaphoreType.DMA((DOWN + 1,)),
            ],
            compiler_params=pltpu.CompilerParams(vmem_limit_bytes=PLACE_VMEM),
            name="place",
        )(y, pltpu.with_memory_space_constraint(kept, pltpu.VMEM))

    return jax.shard_map(
        step,
        mesh=mesh,
        in_specs=(P("dp", None), P(None, "tp"), P(None, "tp"), P("tp", None)),
        out_specs=P("dp", None),
        check_vma=False,
    )
```
